32 devices in a mesh: groups: 2 (over x), ctx: 16 (over z, y, core).
Axes of the slice: x: 2, y: 2, z: 4, core: 2. Of those that a mesh axis runs over, the one named last changes fastest.
Arguments:
- queries: bfloat16 [128, 8192], P(('groups', 'ctx')), parts along dimension 0, may hold values from -200 to 200
- new_kv: bfloat16 [128, 1024], P(('groups', 'ctx')), parts along dimension 0, may hold values from -9 to 9
- prefix_cache: bfloat16 [32768, 1024], P(('groups', 'ctx')), parts along dimension 0, may hold values from -6.5 to 6.5
- positions: int32 [128], P('groups'), parts along dimension 0, may hold values from 0 to 63, each once
- lengths: int32 [32], P('groups'), parts along dimension 0, may hold values from 1 to 1024, 12288 in all
- out_weight: bfloat16 [8192, 16384], P(None, 'ctx'), may hold values from -0.0625 to 0.0625
Outputs:
- attended: bfloat16 [128, 8192], P(('groups', 'ctx')), parts along dimension 0
- projected: bfloat16 [128, 16384], P('groups', 'ctx'), parts along dimension 0
The draws below stay inside these ranges and needn't reach their ends.
There are 2 independent parts, one for each index of `groups`. The reference program is written for one: setup_inputs(seed, part) draws one part's arguments, and reference() takes and returns one part's arrays. A program takes and returns all parts, laid end to end along the dimension named above; an argument that names none is the same for every part. Nothing has to cross between parts.
Inputs may be any that keep to these rules, and one draw needn't show every extreme that they name: `positions`: a permutation of 0 to 63. The filled slots of shard i are its first lengths[i] slots; they sum to 12288, and some shard is full.
All inputs are finite; a program needn't handle non-finite values.
Results may differ from the reference program's by a relative error of at most 0.0045.
Values may be sent and summed in bfloat16 or wider, within the bound.
A program may use at most 128 MiB of HBM per device.

```python
import math
import jax
import jax.numpy as jnp
import numpy as np
from jax import lax

D = 16384
HQ = 64
KVH = 4
HD = 128
BLK = 256
PCAP = 1024
TURN = 64
PREFIX = 12288
N_CTX = 16


def drawn(key):
    base_key = jax.random.fold_in(key, 7101)
    cache_key = jax.random.fold_in(key, 7102)
    scale_key = jax.random.fold_in(key, 7103)
    top_log = math.log(10.0)
    noise = jnp.clip(jax.random.normal(base_key, (TURN, HQ, HD), jnp.float32), -6.0, 6.0)
    head_scales = jnp.exp(jax.random.uniform(scale_key, (TURN, HQ, 1), jnp.float32, 0.0, top_log))
    query_rows = (2.5 * noise * head_scales).reshape(TURN, HQ * HD)
    cache_rows = jnp.clip(jax.random.normal(cache_key, (N_CTX * PCAP, KVH * 2 * HD), jnp.float32), -6.0, 6.0)
    return (query_rows, cache_rows)


def draw_queries(key, part):
    return drawn(key)[0].astype(jnp.bfloat16)


def draw_prefix_cache(key, part):
    return drawn(key)[1].astype(jnp.bfloat16)


def block_levels(key, dims, pieces, low, largest):
    def one(position, shards_of):
        draws = jax.random.uniform(jax.random.fold_in(jax.random.fold_in(key, 6), position), (shards_of,), jnp.float32, low / len(pieces), largest / len(pieces))
        return jnp.repeat(jnp.exp(draws), dims[position] // shards_of).reshape((-1,) + (1,) * (len(dims) - position - 1))

    level = one(*pieces[0])
    for cut in pieces[1:]:
        level = level * one(*cut)
    return level


def split_up(number_of, total, reach, skew):
    weights = [(1 << 20) // math.isqrt(grade ** skew) + 1 for grade in range(2, number_of + 1)]
    surplus, given = total - reach - (number_of - 1), [1] * (number_of - 1)
    while surplus > 0:
        free = [i for i in range(number_of - 1) if given[i] < reach]
        mass, left = sum([weights[i] for i in free]), surplus
        for i in free:
            addition = min(reach - given[i], max(1, left * weights[i] // mass), surplus)
            given[i] = given[i] + addition
            surplus = surplus - addition
    return np.array([reach] + given)


def uneven(stream_key, amount, total, bound, skew):
    if amount == 2:
        one = jax.random.randint(stream_key, (), max(1, total - bound), min(bound, total - 1) + 1)
        return jnp.stack([one, total - one])
    sizes = jnp.asarray(split_up(amount, total, bound, skew), jnp.int32)
    twos = (amount - 1) // 2
    giver, receiver = sizes[1:1 + 2 * twos:2], sizes[2:2 + 2 * twos:2]
    margin = jnp.minimum(giver - 1, bound - receiver)
    passed = jax.random.randint(jax.random.fold_in(stream_key, 1), (twos,), 0, 1 << 20) % (margin + 1)
    sizes = sizes.at[1:1 + 2 * twos:2].set(giver - passed).at[2:2 + 2 * twos:2].set(receiver + passed)
    return sizes[jax.random.permutation(jax.random.fold_in(stream_key, 2), amount)]


def bell_draw(rng, shape, spread, bound, cuts=(), kind=jnp.bfloat16):
    entries = jax.random.normal(rng, shape, jnp.float32) * spread
    if len(cuts) > 0:
        entries = block_levels(rng, shape, cuts, -0.22, 0.18) * entries
    return jnp.clip(entries, min=-bound, max=bound).astype(kind)


def setup_inputs(seed: int = 0, part: int = 0) -> dict:
    streams_of = jax.random.split(jax.random.key(seed), 7)
    part_splits = jax.random.split(jax.random.fold_in(streams_of[6], part), 7)
    return {
        "queries": draw_queries(jax.random.fold_in(jax.random.fold_in(streams_of[6], part), 71), part),
        "new_kv": bell_draw(part_splits[1], (TURN, KVH * 2 * HD), 1.5, 9.0, ((0, 16),)),
        "prefix_cache": draw_prefix_cache(jax.random.fold_in(jax.random.fold_in(streams_of[6], part), 71), part),
        "positions": jax.random.permutation(part_splits[3], TURN).astype(jnp.int32),
        "lengths": uneven(part_splits[4], N_CTX, PREFIX, PCAP, 2).astype(jnp.int32),
        "out_weight": bell_draw(streams_of[5], (HQ * HD, D), (HQ * HD) ** -0.5, 0.0625, ((1, 16),)),
    }


very_low = -1e+30

def block_stats(rows_q, key_rows, values, live_mask):
    scores = jnp.einsum('grd,gkd->grk', rows_q.astype(jnp.float32), key_rows.astype(jnp.float32)) * (1.0 / math.sqrt(HD))
    scores = jnp.where(live_mask, scores, very_low)
    row_max = lax.optimization_barrier(jnp.max(scores, axis=-1))
    weights = jnp.where(live_mask, jnp.exp(scores - row_max[..., None]), 0.0)
    row_total = lax.optimization_barrier(jnp.sum(weights, axis=-1))
    rounded = lax.optimization_barrier(weights.astype(jnp.bfloat16))
    summed = jnp.einsum('grk,gkd->grd', rounded.astype(jnp.float32), values.astype(jnp.float32))
    return (row_max, summed, row_total)

def fold_stats(running, fresh):
    old_max, old_sum, old_total = running
    new_max, new_sum, new_total = fresh
    joint_max = jnp.maximum(old_max, new_max)
    keep_old = jnp.exp(old_max - joint_max)
    keep_new = jnp.exp(new_max - joint_max)
    return (joint_max, old_sum * keep_old[..., None] + new_sum * keep_new[..., None], old_total * keep_old + new_total * keep_new)

def reference(queries, new_kv, prefix_cache, positions, lengths, out_weight):
    per_group = HQ // KVH
    all_rows = TURN * per_group
    group_rows = queries.reshape(TURN, KVH, per_group, HD).transpose(1, 0, 2, 3).reshape(KVH, all_rows, HD)
    block_count = N_CTX * PCAP // BLK
    blocks = prefix_cache.reshape(block_count, BLK, KVH, 2, HD)
    keys_all = blocks[:, :, :, 0].transpose(0, 2, 1, 3)
    values_all = blocks[:, :, :, 1].transpose(0, 2, 1, 3)
    slot_ids = jnp.arange(N_CTX * PCAP, dtype=jnp.int32)
    shard_of = slot_ids // PCAP
    live_all = (slot_ids % PCAP < lengths[shard_of]).reshape(block_count, BLK)
    start_state = (jnp.full((KVH, all_rows), very_low, jnp.float32), jnp.zeros((KVH, all_rows, HD), jnp.float32), jnp.zeros((KVH, all_rows), jnp.float32))

    def step(running, item):
        key_rows, values, live_row = item
        fresh = block_stats(group_rows, key_rows, values, live_row[None, None, :])
        return (fold_stats(running, fresh), None)
    running, _ = lax.scan(step, start_state, (keys_all, values_all, live_all))
    kv_view = new_kv.reshape(TURN, KVH, 2, HD)
    new_keys = kv_view[:, :, 0].transpose(1, 0, 2)
    new_values = kv_view[:, :, 1].transpose(1, 0, 2)
    causal = positions[:, None] >= positions[None, :]
    causal = jnp.repeat(causal, per_group, axis=0)
    fresh = block_stats(group_rows, new_keys, new_values, causal[None])
    combined = fold_stats(running, fresh)
    result = combined[1] / combined[2][..., None]
    attended = result.reshape(KVH, TURN, per_group, HD).transpose(1, 0, 2, 3).reshape(TURN, HQ * HD).astype(jnp.bfloat16)
    projected = jnp.dot(attended, out_weight, preferred_element_type=jnp.float32).astype(jnp.bfloat16)
    return (attended, projected)
```

```python
import functools
import math

import jax
import jax.numpy as jnp
from jax import lax
from jax.experimental import pallas as pl
from jax.experimental.pallas import tpu as pltpu
from jax.sharding import PartitionSpec as P

HQ = 64
KVH = 4
HD = 128
CORES = 2
YN = 2
PAD = 16
STAT = 16
LOW = -1e30
LOG2E = math.log2(math.e)

F32 = jnp.float32
BF16 = jnp.bfloat16


def pack_partial(o, lse):
    hi = lse.astype(BF16).astype(F32)
    mid = (lse - hi).astype(BF16).astype(F32)
    lo = lse - hi - mid
    row = lax.broadcasted_iota(jnp.int32, (STAT, o.shape[1]), 0)
    stat = jnp.where(row == 0, hi, jnp.where(row == 1, mid, lo))
    return jnp.concatenate([o.astype(BF16), stat.astype(BF16)], axis=0)


def unpack_partial(packet):
    stat = packet[HD : HD + STAT].astype(F32)
    return packet[:HD].astype(F32), stat[0:1] + stat[1:2] + stat[2:3]


def merge_partials(parts):
    top = functools.reduce(jnp.maximum, [lse for _, lse in parts])
    weights = [jnp.exp2(lse - top) for _, lse in parts]
    total = functools.reduce(jnp.add, weights)
    inverse = 1.0 / total
    out = functools.reduce(
        jnp.add, [o * (w * inverse) for (o, _), w in zip(parts, weights)]
    )
    return out, top + jnp.log(total) * LOG2E


def kernel(
    n,
    positions,
    lengths,
    q_ref,
    nk_ref,
    cache,
    weight,
    att_out,
    proj_out,
    wv,
    kvx,
    vt,
    nkx,
    qd,
    qall,
    sc,
    pk,
    ry,
    zm,
    rz,
    ag,
    a_ref,
    acc,
    w_sem,
    kv_sem,
    kvs_sem,
    kvr_sem,
    nk_sem,
    nks_sem,
    nkr_sem,
    qd_sem,
    qds_sem,
    qdr_sem,
    qz_s,
    qz_r,
    qy_s,
    qy_r,
    ry_s,
    ry_r,
    rz_s,
    rz_r,
    gz_s,
    gz_r,
    gy_s,
    gy_r,
    gc_s,
    gc_r,
):
    zn = n // (YN * CORES)
    me = lax.axis_index("ctx")
    c = lax.rem(me, CORES)
    chip = me // CORES
    y = lax.rem(chip, YN)
    z = chip // YN
    oc = 1 - c
    oy = 1 - y
    jn = KVH // CORES
    per = HQ // KVH
    td = q_ref.shape[0]
    ct = td * CORES
    rows = per * ct
    lanes = YN * rows
    slots = cache.shape[0]
    gw = 2 * HD
    half = HQ // CORES * HD
    wide = per * HD
    ch = min(512, slots)
    units = jn * zn
    c2 = LOG2E / math.sqrt(HD)

    def zat(d):
        return lax.rem(z + d, zn)

    def zsrc(d):
        return lax.rem(z - d + zn, zn)

    def dev(zz, yy, cc):
        return {"ctx": (zz * YN + yy) * CORES + cc}

    peer = dev(z, y, oc)
    ypart = dev(z, oy, c)

    def remote(src, dst, ssem, rsem, target):
        return pltpu.make_async_remote_copy(
            src_ref=src,
            dst_ref=dst,
            send_sem=ssem,
            recv_sem=rsem,
            device_id=target,
            device_id_type=pl.DeviceIdType.MESH,
        )

    def arrived(slot, sem):
        pltpu.make_async_copy(slot, slot, sem).wait()

    def cols(group):
        return pl.ds(pl.multiple_of(group * gw, gw), gw)

    local = []
    for j in range(jn):
        local.append(
            pltpu.make_async_copy(cache.at[:, cols(c * jn + j)], kvx.at[j, c], kv_sem.at[j])
        )
    for j in range(jn):
        local.append(
            pltpu.make_async_copy(nk_ref.at[:, cols(c * jn + j)], nkx.at[j, c], nk_sem.at[j])
        )
    q_half = pl.ds(pl.multiple_of(c * half, half), half)
    q_other = pl.ds(pl.multiple_of(oc * half, half), half)
    q_local = pltpu.make_async_copy(q_ref.at[:, q_half], qd.at[c], qd_sem)
    q_local.start()
    for copy in local:
        copy.start()

    barrier = pltpu.get_barrier_semaphore()
    pl.semaphore_signal(barrier, inc=1, device_id=peer, device_id_type=pl.DeviceIdType.MESH)
    pl.semaphore_signal(barrier, inc=1, device_id=ypart, device_id_type=pl.DeviceIdType.MESH)
    for d in range(1, zn):
        pl.semaphore_signal(
            barrier, inc=1, device_id=dev(zat(d), y, c), device_id_type=pl.DeviceIdType.MESH
        )
    pl.semaphore_wait(barrier, zn + 1)

    sends = []

    def send(*args):
        copy = remote(*args)
        copy.start()
        sends.append(copy)

    send(q_ref.at[:, q_other], qd.at[c], qds_sem, qdr_sem, peer)
    for j in range(jn):
        send(nk_ref.at[:, cols(oc * jn + j)], nkx.at[j, c], nks_sem.at[j], nkr_sem.at[j], peer)
        send(cache.at[:, cols(oc * jn + j)], kvx.at[j, c], kvs_sem.at[j], kvr_sem.at[j], peer)
    weights = []
    for j in range(jn):
        for k in range(CORES):
            g = k * jn + j
            copy = pltpu.make_async_copy(
                weight.at[pl.ds(g * wide, wide), :], wv.at[g], w_sem.at[g]
            )
            copy.start()
            weights.append(copy)

    q_local.wait()
    arrived(qd.at[oc], qdr_sem)
    my_rows = pl.ds(pl.multiple_of(y * rows, rows), rows)
    other_rows = pl.ds(pl.multiple_of(oy * rows, rows), rows)
    for j in range(jn):
        tiles = []
        for h in range(per):
            at = (j * per + h) * HD
            tiles.append(
                jnp.concatenate(
                    [qd[k, :, at : at + HD].astype(F32) for k in range(CORES)], axis=0
                )
            )
        qall[z, j, my_rows, :] = jnp.concatenate(tiles, axis=0).astype(BF16)

    mine = qall.at[z, :, my_rows]
    send(mine, mine, qy_s.at[0], qy_r.at[0], ypart)
    for d in range(1, zn):
        send(mine, mine, qz_s.at[d], qz_r.at[d], dev(zat(d), y, c))

    for j in range(jn):
        local[j].wait()
        local[jn + j].wait()
        arrived(nkx.at[j, oc], nkr_sem.at[j])
        arrived(kvx.at[j, oc], kvr_sem.at[j])
        for k in range(CORES):
            vt[j, k] = kvx[j, k, :, HD:].T
    arrived(qall.at[z, :, other_rows], qy_r.at[0])

    def attend(j, d):
        zz = zsrc(d)
        q = qall[zz, j]
        lane = lax.broadcasted_iota(jnp.int32, (1, lanes), 1)
        token = lax.rem(lane, ct) + (lane // rows) * ct
        pos = jnp.zeros((1, lanes), jnp.int32)
        for t in range(YN * ct):
            pos = jnp.where(token == t, positions[zz * (YN * ct) + t], pos)
        top = jnp.full((8, lanes), LOW, F32)
        for k in range(CORES):
            live = lengths[chip * CORES + k]
            for i in range(slots // ch):
                s = lax.dot_general(
                    kvx[j, k, i * ch : (i + 1) * ch, :HD],
                    q,
                    (((1,), (1,)), ((), ())),
                    preferred_element_type=F32,
                )
                slot = lax.broadcasted_iota(jnp.int32, s.shape, 0)
                s = jnp.where(slot < live - i * ch, s, LOW)
                top = jnp.maximum(top, jnp.max(s.reshape(ch // 8, 8, lanes), axis=0))
                at = k * slots + i * ch
                sc[at : at + ch, :] = s
        row = lax.broadcasted_iota(jnp.int32, (PAD, lanes), 0)
        fresh = []
        for k in range(CORES):
            s = lax.dot_general(
                nkx[j, k, :, :HD], q, (((1,), (1,)), ((), ())), preferred_element_type=F32
            )
            key_pos = jnp.full((PAD, lanes), jnp.int32(2**30))
            for t in range(td):
                key_pos = jnp.where(row == t, positions[chip * ct + k * td + t], key_pos)
            s = jnp.where(pos >= key_pos, s, LOW)
            top = jnp.maximum(top, jnp.max(s.reshape(PAD // 8, 8, lanes), axis=0))
            fresh.append(s)
        high = jnp.max(top, axis=0, keepdims=True) * c2
        total = jnp.zeros((8, lanes), F32)
        out = jnp.zeros((HD, lanes), F32)
        for k in range(CORES):
            for i in range(slots // ch):
                at = k * slots + i * ch
                p = jnp.exp2(sc[at : at + ch, :] * c2 - high)
                total = total + jnp.sum(p.reshape(ch // 8, 8, lanes), axis=0)
                out = out + jnp.dot(
                    vt[j, k, :, i * ch : (i + 1) * ch],
                    p.astype(BF16),
                    preferred_element_type=F32,
                )
        for k in range(CORES):
            p = jnp.exp2(fresh[k] * c2 - high)
            total = total + jnp.sum(p.reshape(PAD // 8, 8, lanes), axis=0)
            out = out + lax.dot_general(
                nkx[j, k, :, HD:],
                p.astype(BF16),
                (((0,), (0,)), ((), ())),
                preferred_element_type=F32,
            )
        ell = jnp.sum(total, axis=0, keepdims=True)
        packet = pack_partial(out * (1.0 / ell), high + jnp.log(ell) * LOG2E)
        u = j * zn + d
        for yy in range(YN):
            pk[u, yy] = packet[:, yy * rows : (yy + 1) * rows]
        to_partner(u).start()

    def to_partner(u):
        return remote(pk.at[u, oy], ry.at[u], ry_s.at[u], ry_r.at[u], ypart)

    def to_owner(u, d):
        return remote(zm.at[u], rz.at[u], rz_s.at[u], rz_r.at[u], dev(zsrc(d), y, c))

    def fold(j, d):
        u = j * zn + d
        arrived(ry.at[u], ry_r.at[u])
        packet = pack_partial(
            *merge_partials([unpack_partial(pk[u, y]), unpack_partial(ry[u])])
        )

        @pl.when(d == 0)
        def _():
            rz[u] = packet

        @pl.when(d != 0)
        def _():
            zm[u] = packet
            to_owner(u, d).start()

    def relay_queries():
        for d in range(1, zn):
            slot = qall.at[zsrc(d), :, my_rows]
            arrived(slot, qz_r.at[d])
            send(slot, slot, qy_s.at[d], qy_r.at[d], ypart)

    def finish(j):
        for d in range(1, zn):
            arrived(rz.at[j * zn + d], rz_r.at[j * zn + d])
        out, _ = merge_partials([unpack_partial(rz[j * zn + d]) for d in range(zn)])
        out = out.T
        for h in range(per):
            ag[c, j, chip, :, h * HD : (h + 1) * HD] = out[h * ct : (h + 1) * ct].astype(BF16)
        slot = ag.at[c, j, chip]
        for d in range(1, zn):
            send(slot, slot, gz_s.at[j, d], gz_r.at[j, d], dev(zat(d), y, c))
        send(slot, slot, gy_s.at[j, 0], gy_r.at[j, 0], ypart)
        send(slot, slot, gc_s.at[j, 0, 0], gc_r.at[j, 0, 0], peer)

    def relay_outputs(j):
        for d in range(1, zn):
            slot = ag.at[c, j, zsrc(d) * YN + y]
            arrived(slot, gz_r.at[j, d])
            send(slot, slot, gy_s.at[j, d], gy_r.at[j, d], ypart)
            send(slot, slot, gc_s.at[j, 0, d], gc_r.at[j, 0, d], peer)
        for d in range(zn):
            slot = ag.at[c, j, zsrc(d) * YN + oy]
            arrived(slot, gy_r.at[j, d])
            send(slot, slot, gc_s.at[j, 1, d], gc_r.at[j, 1, d], peer)

    def project(j):
        for d in range(zn):
            arrived(ag.at[oc, j, zsrc(d) * YN + y], gc_r.at[j, 0, d])
            arrived(ag.at[oc, j, zsrc(d) * YN + oy], gc_r.at[j, 1, d])
        width = proj_out.shape[1]
        nb = min(256, width)
        for k in range(CORES):
            g = k * jn + j
            weights[j * CORES + k].wait()
            whole = jnp.concatenate(
                [ag[k, j, i].astype(F32) for i in range(zn * YN)], axis=0
            )
            a_ref[k] = whole.astype(BF16)
            own = ag[k, j, chip].astype(F32)
            own = jnp.where(c == 0, own[:td], own[td:])
            att_out[:, g * wide : (g + 1) * wide] = own.astype(BF16)

        def column(i, carry):
            at = pl.ds(pl.multiple_of(i * nb, nb), nb)
            part = jnp.dot(a_ref[0], wv[j, :, at], preferred_element_type=F32)
            for k in range(1, CORES):
                part = part + jnp.dot(
                    a_ref[k], wv[k * jn + j, :, at], preferred_element_type=F32
                )
            if j > 0:
                part = part + acc[:, at]
            if j == jn - 1:
                proj_out[:, at] = part.astype(BF16)
            else:
                acc[:, at] = part
            return carry

        lax.fori_loop(0, width // nb, column, 0)

    def step(u, carry):
        j = u // zn
        d = lax.rem(u, zn)

        @pl.when((u > 0) & (u < zn))
        def _():
            slot = qall.at[zsrc(d), :, other_rows]
            arrived(slot, qy_r.at[d])

        attend(j, d)

        @pl.when(u > 0)
        def _():
            fold((u - 1) // zn, lax.rem(u - 1, zn))

        return carry

    lax.fori_loop(0, 1, step, 0)
    relay_queries()
    lax.fori_loop(1, units, step, 0)
    fold(jn - 1, zn - 1)
    for j in range(jn):
        finish(j)
    for j in range(jn):
        relay_outputs(j)
    for j in range(jn):
        project(j)

    for copy in sends:
        copy.wait_send()

    def drain(u, carry):
        to_partner(u).wait_send()
        d = lax.rem(u, zn)

        @pl.when(d != 0)
        def _():
            to_owner(u, d).wait_send()

        return carry

    lax.fori_loop(0, units, drain, 0)


def shards(queries, new_kv, prefix_cache, positions, lengths, out_weight):
    n = lax.axis_size("ctx")
    td = queries.shape[0]
    zn = n // (YN * CORES)
    jn = KVH // CORES
    per = HQ // KVH
    ct = td * CORES
    rows = per * ct
    slots = prefix_cache.shape[0]
    width = out_weight.shape[1]
    wide = per * HD
    units = jn * zn
    dma = pltpu.SemaphoreType.DMA
    scratch = [
        pltpu.VMEM((KVH, wide, width), BF16),
        pltpu.VMEM((jn, CORES, slots, 2 * HD), BF16),
        pltpu.VMEM((jn, CORES, HD, slots), BF16),
        pltpu.VMEM((jn, CORES, PAD, 2 * HD), BF16),
        pltpu.VMEM((CORES, td, HQ // CORES * HD), BF16),
        pltpu.VMEM((zn, jn, YN * rows, HD), BF16),
        pltpu.VMEM((CORES * slots, YN * rows), F32),
        pltpu.VMEM((units, YN, HD + STAT, rows), BF16),
        pltpu.VMEM((units, HD + STAT, rows), BF16),
        pltpu.VMEM((units, HD + STAT, rows), BF16),
        pltpu.VMEM((units, HD + STAT, rows), BF16),
        pltpu.VMEM((CORES, jn, zn * YN, ct, wide), BF16),
        pltpu.VMEM((CORES, td * n, wide), BF16),
        pltpu.VMEM((td * n, width), F32),
        dma((KVH,)),
        dma((jn,)),
        dma((jn,)),
        dma((jn,)),
        dma((jn,)),
        dma((jn,)),
        dma((jn,)),
        dma,
        dma,
        dma,
        dma((zn,)),
        dma((zn,)),
        dma((zn,)),
        dma((zn,)),
        dma((units,)),
        dma((units,)),
        dma((units,)),
        dma((units,)),
        dma((jn, zn)),
        dma((jn, zn)),
        dma((jn, zn)),
        dma((jn, zn)),
        dma((jn, YN, zn)),
        dma((jn, YN, zn)),
    ]
    padded = jnp.pad(new_kv, ((0, PAD - td), (0, 0)))
    smem = pl.BlockSpec(memory_space=pltpu.SMEM)
    vmem = pl.BlockSpec(memory_space=pltpu.VMEM)
    hbm = pl.BlockSpec(memory_space=pl.ANY)
    return pl.pallas_call(
        functools.partial(kernel, n),
        out_shape=(
            jax.ShapeDtypeStruct(queries.shape, BF16),
            jax.ShapeDtypeStruct((td * n, width), BF16),
        ),
        in_specs=[smem, smem, vmem, vmem, hbm, hbm],
        out_specs=(vmem, vmem),
        scratch_shapes=scratch,
        compiler_params=pltpu.CompilerParams(
            collective_id=0,
            has_side_effects=True,
            vmem_limit_bytes=60 * 2**20,
        ),
        name="turn_attention",
    )(positions, lengths, queries, padded, prefix_cache, out_weight)


def solution(mesh):
    in_specs = (
        P(("groups", "ctx"), None),
        P(("groups", "ctx"), None),
        P(("groups", "ctx"), None),
        P("groups"),
        P("groups"),
        P(None, "ctx"),
    )
    out_specs = (P(("groups", "ctx"), None), P("groups", "ctx"))
    return jax.shard_map(shards, mesh=mesh, in_specs=in_specs, out_specs=out_specs, check_vma=False)
```

```python
import functools
import math

import jax
import jax.numpy as jnp
from jax import lax
from jax.experimental import pallas as pl
from jax.experimental.pallas import tpu as pltpu
from jax.sharding import PartitionSpec as P

HQ = 64
KVH = 4
HD = 128
CORES = 2
YN = 2
PAD = 16
STAT = 16
LOW = -1e30
LOG2E = math.log2(math.e)

F32 = jnp.float32
BF16 = jnp.bfloat16


def pack_partial(o, lse):
    hi = lse.astype(BF16).astype(F32)
    mid = (lse - hi).astype(BF16).astype(F32)
    lo = lse - hi - mid
    row = lax.broadcasted_iota(jnp.int32, (STAT, o.shape[1]), 0)
    stat = jnp.where(row == 0, hi, jnp.where(row == 1, mid, lo))
    return jnp.concatenate([o.astype(BF16), stat.astype(BF16)], axis=0)


def unpack_partial(packet):
    stat = packet[HD : HD + STAT].astype(F32)
    return packet[:HD].astype(F32), stat[0:1] + stat[1:2] + stat[2:3]


def merge_partials(parts):
    top = functools.reduce(jnp.maximum, [lse for _, lse in parts])
    weights = [jnp.exp2(lse - top) for _, lse in parts]
    total = functools.reduce(jnp.add, weights)
    inverse = 1.0 / total
    out = functools.reduce(
        jnp.add, [o * (w * inverse) for (o, _), w in zip(parts, weights)]
    )
    return out, top + jnp.log(total) * LOG2E


def kernel(
    n,
    positions,
    lengths,
    q_ref,
    nk_ref,
    cache,
    weight,
    att_out,
    proj_out,
    wv,
    kvx,
    vt,
    nkx,
    nkp,
    qd,
    qall,
    sc,
    pk,
    ry,
    zm,
    rz,
    ag,
    a_ref,
    acc,
    w_sem,
    kv_sem,
    kvs_sem,
    kvr_sem,
    nk_sem,
    nks_sem,
    nkr_sem,
    qd_sem,
    qds_sem,
    qdr_sem,
    qz_s,
    qz_r,
    qy_s,
    qy_r,
    ry_s,
    ry_r,
    rz_s,
    rz_r,
    gz_s,
    gz_r,
    gy_s,
    gy_r,
    gc_s,
    gc_r,
):
    zn = n // (YN * CORES)
    me = lax.axis_index("ctx")
    c = lax.rem(me, CORES)
    chip = me // CORES
    y = lax.rem(chip, YN)
    z = chip // YN
    oc = 1 - c
    oy = 1 - y
    jn = KVH // CORES
    per = HQ // KVH
    td = q_ref.shape[0]
    ct = td * CORES
    rows = per * ct
    lanes = YN * rows
    slots = cache.shape[0]
    gw = 2 * HD
    half = HQ // CORES * HD
    wide = per * HD
    ch = min(512, slots)
    units = jn * zn
    c2 = LOG2E / math.sqrt(HD)

    def zat(d):
        if zn & (zn - 1):
            return lax.rem(z + d, zn)
        out = 0
        for bit in range(zn.bit_length() - 1):
            step = 1 << bit
            out = out + lax.rem(z // step + d // step, 2) * step
        return out

    def zsrc(d):
        if zn & (zn - 1):
            return lax.rem(z - d + zn, zn)
        return zat(d)

    def dev(zz, yy, cc):
        return {"ctx": (zz * YN + yy) * CORES + cc}

    peer = dev(z, y, oc)
    ypart = dev(z, oy, c)

    def remote(src, dst, ssem, rsem, target):
        return pltpu.make_async_remote_copy(
            src_ref=src,
            dst_ref=dst,
            send_sem=ssem,
            recv_sem=rsem,
            device_id=target,
            device_id_type=pl.DeviceIdType.MESH,
        )

    def arrived(slot, sem):
        pltpu.make_async_copy(slot, slot, sem).wait()

    def cols(group):
        return pl.ds(pl.multiple_of(group * gw, gw), gw)

    local = []
    for j in range(jn):
        local.append(
            pltpu.make_async_copy(cache.at[:, cols(c * jn + j)], kvx.at[j, c], kv_sem.at[j])
        )
    for j in range(jn):
        local.append(
            pltpu.make_async_copy(nk_ref.at[:, cols(c * jn + j)], nkx.at[j, c], nk_sem.at[j])
        )
    q_half = pl.ds(pl.multiple_of(c * half, half), half)
    q_other = pl.ds(pl.multiple_of(oc * half, half), half)
    q_local = pltpu.make_async_copy(q_ref.at[:, q_half], qd.at[c], qd_sem)
    q_local.start()
    for copy in local:
        copy.start()

    barrier = pltpu.get_barrier_semaphore()
    pl.semaphore_signal(barrier, inc=1, device_id=peer, device_id_type=pl.DeviceIdType.MESH)
    pl.semaphore_signal(barrier, inc=1, device_id=ypart, device_id_type=pl.DeviceIdType.MESH)
    for d in range(1, zn):
        pl.semaphore_signal(
            barrier, inc=1, device_id=dev(zat(d), y, c), device_id_type=pl.DeviceIdType.MESH
        )
    pl.semaphore_wait(barrier, zn + 1)

    sends = []

    def send(*args):
        copy = remote(*args)
        copy.start()
        sends.append(copy)

    send(q_ref.at[:, q_other], qd.at[c], qds_sem, qdr_sem, peer)
    for j in range(jn):
        send(nk_ref.at[:, cols(oc * jn + j)], nkx.at[j, c], nks_sem.at[j], nkr_sem.at[j], peer)
        send(cache.at[:, cols(oc * jn + j)], kvx.at[j, c], kvs_sem.at[j], kvr_sem.at[j], peer)
    weights = []
    for j in range(jn):
        for k in range(CORES):
            g = k * jn + j
            copy = pltpu.make_async_copy(
                weight.at[pl.ds(g * wide, wide), :], wv.at[g], w_sem.at[g]
            )
            copy.start()
            weights.append(copy)

    q_local.wait()
    arrived(qd.at[oc], qdr_sem)
    my_rows = pl.ds(pl.multiple_of(y * rows, rows), rows)
    other_rows = pl.ds(pl.multiple_of(oy * rows, rows), rows)
    for j in range(jn):
        tiles = []
        for h in range(per):
            at = (j * per + h) * HD
            tiles.append(
                jnp.concatenate(
                    [qd[k, :, at : at + HD].astype(F32) for k in range(CORES)], axis=0
                )
            )
        qall[z, j, my_rows, :] = jnp.concatenate(tiles, axis=0).astype(BF16)

    mine = qall.at[z, :, my_rows]
    send(mine, mine, qy_s.at[0], qy_r.at[0], ypart)
    for d in range(1, zn):
        send(mine, mine, qz_s.at[d], qz_r.at[d], dev(zat(d), y, c))

    for j in range(jn):
        local[j].wait()
        local[jn + j].wait()
        arrived(nkx.at[j, oc], nkr_sem.at[j])
        fresh = [nkx[j, k].astype(F32) for k in range(CORES)]
        fresh.append(jnp.zeros((PAD - ct, gw), F32))
        nkp[j] = jnp.concatenate(fresh, axis=0).astype(BF16)
        arrived(kvx.at[j, oc], kvr_sem.at[j])
        for k in range(CORES):
            vt[j, k] = kvx[j, k, :, HD:].T

    def attend(j, d):
        zz = zsrc(d)
        q = qall[zz, j]
        lane = lax.broadcasted_iota(jnp.int32, (1, lanes), 1)
        token = lax.rem(lane, ct) + (lane // rows) * ct
        pos = jnp.zeros((1, lanes), jnp.int32)
        for t in range(YN * ct):
            pos = jnp.where(token == t, positions[zz * (YN * ct) + t], pos)
        top = jnp.full((8, lanes), LOW, F32)
        for k in range(CORES):
            live = lengths[chip * CORES + k]
            for i in range(slots // ch):
                s = lax.dot_general(
                    kvx[j, k, i * ch : (i + 1) * ch, :HD],
                    q,
                    (((1,), (1,)), ((), ())),
                    preferred_element_type=F32,
                )
                slot = lax.broadcasted_iota(jnp.int32, s.shape, 0)
                s = jnp.where(slot < live - i * ch, s, LOW)
                top = jnp.maximum(top, jnp.max(s.reshape(ch // 8, 8, lanes), axis=0))
                at = k * slots + i * ch
                sc[at : at + ch, :] = s
        row = lax.broadcasted_iota(jnp.int32, (PAD, lanes), 0)
        fresh = lax.dot_general(
            nkp[j, :, :HD], q, (((1,), (1,)), ((), ())), preferred_element_type=F32
        )
        key_pos = jnp.full((PAD, lanes), jnp.int32(2**30))
        for t in range(ct):
            key_pos = jnp.where(row == t, positions[chip * ct + t], key_pos)
        fresh = jnp.where(pos >= key_pos, fresh, LOW)
        top = jnp.maximum(top, jnp.max(fresh.reshape(PAD // 8, 8, lanes), axis=0))
        high = jnp.max(top, axis=0, keepdims=True) * c2
        total = jnp.zeros((8, lanes), F32)
        out = jnp.zeros((HD, lanes), F32)
        for k in range(CORES):
            for i in range(slots // ch):
                at = k * slots + i * ch
                p = jnp.exp2(sc[at : at + ch, :] * c2 - high)
                total = total + jnp.sum(p.reshape(ch // 8, 8, lanes), axis=0)
                out = out + jnp.dot(
                    vt[j, k, :, i * ch : (i + 1) * ch],
                    p.astype(BF16),
                    preferred_element_type=F32,
                )
        p = jnp.exp2(fresh * c2 - high)
        total = total + jnp.sum(p.reshape(PAD // 8, 8, lanes), axis=0)
        out = out + lax.dot_general(
            nkp[j, :, HD:],
            p.astype(BF16),
            (((0,), (0,)), ((), ())),
            preferred_element_type=F32,
        )
        ell = jnp.sum(total, axis=0, keepdims=True)
        packet = pack_partial(out * (1.0 / ell), high + jnp.log(ell) * LOG2E)
        u = j * zn + d
        for yy in range(YN):
            pk[u, yy] = packet[:, yy * rows : (yy + 1) * rows]
        to_partner(u).start()

    def to_partner(u):
        return remote(pk.at[u, oy], ry.at[u], ry_s.at[u], ry_r.at[u], ypart)

    def to_owner(u, d):
        return remote(zm.at[u], rz.at[u], rz_s.at[u], rz_r.at[u], dev(zsrc(d), y, c))

    def fold(j, d):
        u = j * zn + d
        arrived(ry.at[u], ry_r.at[u])
        packet = pack_partial(
            *merge_partials([unpack_partial(pk[u, y]), unpack_partial(ry[u])])
        )

        if isinstance(d, int) and d == 0:
            rz[u] = packet
            return

        @pl.when(d == 0)
        def _():
            rz[u] = packet

        @pl.when(d != 0)
        def _():
            zm[u] = packet
            to_owner(u, d).start()

    def query_relay(d):
        slot = qall.at[zsrc(d), :, my_rows]
        return remote(slot, slot, qy_s.at[d], qy_r.at[d], ypart)

    def relay_query(d):
        arrived(qall.at[zsrc(d), :, my_rows], qz_r.at[d])
        query_relay(d).start()

    def finish(j):
        for d in range(1, zn):
            arrived(rz.at[j * zn + d], rz_r.at[j * zn + d])
        out, _ = merge_partials([unpack_partial(rz[j * zn + d]) for d in range(zn)])
        out = out.T
        for h in range(per):
            ag[c, j, chip, :, h * HD : (h + 1) * HD] = out[h * ct : (h + 1) * ct].astype(BF16)
        slot = ag.at[c, j, chip]
        for d in range(1, zn):
            send(slot, slot, gz_s.at[j, d], gz_r.at[j, d], dev(zat(d), y, c))
        send(slot, slot, gy_s.at[j, 0], gy_r.at[j, 0], ypart)
        send(slot, slot, gc_s.at[j, 0, 0], gc_r.at[j, 0, 0], peer)

    def relay_along(j):
        for d in range(1, zn):
            slot = ag.at[c, j, zsrc(d) * YN + y]
            arrived(slot, gz_r.at[j, d])
            send(slot, slot, gy_s.at[j, d], gy_r.at[j, d], ypart)
            send(slot, slot, gc_s.at[j, 0, d], gc_r.at[j, 0, d], peer)

    def relay_across(j):
        for d in range(zn):
            slot = ag.at[c, j, zsrc(d) * YN + oy]
            arrived(slot, gy_r.at[j, d])
            send(slot, slot, gc_s.at[j, 1, d], gc_r.at[j, 1, d], peer)

    def project(j, k, first, last):
        width = proj_out.shape[1]
        nb = min(256, width)
        g = k * jn + j
        whole = jnp.concatenate([ag[k, j, i].astype(F32) for i in range(zn * YN)], axis=0)
        a_ref[...] = whole.astype(BF16)
        own = ag[k, j, chip].astype(F32)
        own = jnp.where(c == 0, own[:td], own[td:])
        att_out[:, pl.ds(pl.multiple_of(g * wide, wide), wide)] = own.astype(BF16)

        def column(i, carry):
            at = pl.ds(pl.multiple_of(i * nb, nb), nb)
            part = jnp.dot(a_ref[...], wv[g, :, at], preferred_element_type=F32)
            if not first:
                part = part + acc[:, at]
            if last:
                proj_out[:, at] = part.astype(BF16)
            else:
                acc[:, at] = part
            return carry

        lax.fori_loop(0, width // nb, column, 0)

    def project_both(j):
        if j == 0:
            for copy in weights:
                copy.wait()
        project(j, c, j == 0, False)
        for d in range(zn):
            arrived(ag.at[oc, j, zsrc(d) * YN + y], gc_r.at[j, 0, d])
            arrived(ag.at[oc, j, zsrc(d) * YN + oy], gc_r.at[j, 1, d])
        project(j, oc, False, j == jn - 1)

    relay_query(1)
    arrived(qall.at[z, :, other_rows], qy_r.at[0])
    attend(0, 0)
    relay_query(2)
    attend(1, 0)
    for d in range(3, zn):
        relay_query(d)

    def first_group(d, carry):
        arrived(qall.at[zsrc(d), :, other_rows], qy_r.at[d])
        attend(0, d)

        @pl.when(d >= 2)
        def _():
            fold(0, d - 2)

        return carry

    def second_group(d, carry):
        attend(1, d)

        @pl.when(d == 1)
        def _():
            fold(0, zn - 2)
            fold(0, zn - 1)

        @pl.when(d == 2)
        def _():
            fold(1, 0)

        @pl.when(d >= 3)
        def _():
            fold(1, d - 2)

        return carry

    lax.fori_loop(1, zn, first_group, 0)
    lax.fori_loop(1, zn, second_group, 0)
    finish(0)
    fold(1, zn - 2)
    fold(1, zn - 1)
    relay_along(0)
    finish(1)
    relay_across(0)
    relay_along(1)
    project_both(0)
    relay_across(1)
    project_both(1)

    for copy in sends:
        copy.wait_send()

    def drain(u, carry):
        to_partner(u).wait_send()
        d = lax.rem(u, zn)

        @pl.when(d != 0)
        def _():
            to_owner(u, d).wait_send()

        @pl.when((u > 0) & (u < zn))
        def _():
            query_relay(d).wait_send()

        return carry

    lax.fori_loop(0, units, drain, 0)


def shards(queries, new_kv, prefix_cache, positions, lengths, out_weight):
    n = lax.axis_size("ctx")
    td = queries.shape[0]
    zn = n // (YN * CORES)
    jn = KVH // CORES
    per = HQ // KVH
    ct = td * CORES
    rows = per * ct
    slots = prefix_cache.shape[0]
    width = out_weight.shape[1]
    wide = per * HD
    units = jn * zn
    dma = pltpu.SemaphoreType.DMA
    scratch = [
        pltpu.VMEM((KVH, wide, width), BF16),
        pltpu.VMEM((jn, CORES, slots, 2 * HD), BF16),
        pltpu.VMEM((jn, CORES, HD, slots), BF16),
        pltpu.VMEM((jn, CORES, td, 2 * HD), BF16),
        pltpu.VMEM((jn, PAD, 2 * HD), BF16),
        pltpu.VMEM((CORES, td, HQ // CORES * HD), BF16),
        pltpu.VMEM((zn, jn, YN * rows, HD), BF16),
        pltpu.VMEM((CORES * slots, YN * rows), F32),
        pltpu.VMEM((units, YN, HD + STAT, rows), BF16),
        pltpu.VMEM((units, HD + STAT, rows), BF16),
        pltpu.VMEM((units, HD + STAT, rows), BF16),
        pltpu.VMEM((units, HD + STAT, rows), BF16),
        pltpu.VMEM((CORES, jn, zn * YN, ct, wide), BF16),
        pltpu.VMEM((td * n, wide), BF16),
        pltpu.VMEM((td * n, width), F32),
        dma((KVH,)),
        dma((jn,)),
        dma((jn,)),
        dma((jn,)),
        dma((jn,)),
        dma((jn,)),
        dma((jn,)),
        dma,
        dma,
        dma,
        dma((zn,)),
        dma((zn,)),
        dma((zn,)),
        dma((zn,)),
        dma((units,)),
        dma((units,)),
        dma((units,)),
        dma((units,)),
        dma((jn, zn)),
        dma((jn, zn)),
        dma((jn, zn)),
        dma((jn, zn)),
        dma((jn, YN, zn)),
        dma((jn, YN, zn)),
    ]
    smem = pl.BlockSpec(memory_space=pltpu.SMEM)
    vmem = pl.BlockSpec(memory_space=pltpu.VMEM)
    hbm = pl.BlockSpec(memory_space=pl.ANY)
    return pl.pallas_call(
        functools.partial(kernel, n),
        out_shape=(
            jax.ShapeDtypeStruct(queries.shape, BF16),
            jax.ShapeDtypeStruct((td * n, width), BF16),
        ),
        in_specs=[smem, smem, vmem, vmem, hbm, hbm],
        out_specs=(vmem, vmem),
        scratch_shapes=scratch,
        compiler_params=pltpu.CompilerParams(
            collective_id=0,
            has_side_effects=True,
            vmem_limit_bytes=60 * 2**20,
        ),
        name="turn_attention",
    )(positions, lengths, queries, new_kv, prefix_cache, out_weight)


def solution(mesh):
    in_specs = (
        P(("groups", "ctx"), None),
        P(("groups", "ctx"), None),
        P(("groups", "ctx"), None),
        P("groups"),
        P("groups"),
        P(None, "ctx"),
    )
    out_specs = (P(("groups", "ctx"), None), P("groups", "ctx"))
    return jax.shard_map(shards, mesh=mesh, in_specs=in_specs, out_specs=out_specs, check_vma=False)
```

```python
import functools
import math

import jax
import jax.numpy as jnp
from jax import lax
from jax.experimental import pallas as pl
from jax.experimental.pallas import tpu as pltpu
from jax.sharding import PartitionSpec as P

HQ = 64
KVH = 4
HD = 128
CORES = 2
YN = 2
PAD = 16
STAT = 16
LOW = -1e30
LOG2E = math.log2(math.e)

F32 = jnp.float32
BF16 = jnp.bfloat16


def pack_partial(o, lse):
    hi = lse.astype(BF16).astype(F32)
    mid = (lse - hi).astype(BF16).astype(F32)
    lo = lse - hi - mid
    row = lax.broadcasted_iota(jnp.int32, (STAT, o.shape[1]), 0)
    stat = jnp.where(row == 0, hi, jnp.where(row == 1, mid, lo))
    return jnp.concatenate([o.astype(BF16), stat.astype(BF16)], axis=0)


def unpack_partial(packet):
    stat = packet[HD : HD + STAT].astype(F32)
    return packet[:HD].astype(F32), stat[0:1] + stat[1:2] + stat[2:3]


def merge_partials(parts):
    top = functools.reduce(jnp.maximum, [lse for _, lse in parts])
    weights = [jnp.exp2(lse - top) for _, lse in parts]
    total = functools.reduce(jnp.add, weights)
    inverse = 1.0 / total
    out = functools.reduce(
        jnp.add, [o * (w * inverse) for (o, _), w in zip(parts, weights)]
    )
    return out, top + jnp.log(total) * LOG2E


def kernel(
    n,
    positions,
    lengths,
    q_ref,
    nk_ref,
    cache,
    weight,
    att_out,
    proj_out,
    wv,
    kvx,
    vt,
    nkx,
    nkp,
    qd,
    qall,
    sc,
    pk,
    ry,
    zm,
    rz,
    ag,
    a_ref,
    acc,
    w_sem,
    kv_sem,
    kvs_sem,
    kvr_sem,
    nk_sem,
    nks_sem,
    nkr_sem,
    qd_sem,
    qds_sem,
    qdr_sem,
    qz_s,
    qz_r,
    qy_s,
    qy_r,
    ry_s,
    ry_r,
    rz_s,
    rz_r,
    gz_s,
    gz_r,
    gy_s,
    gy_r,
    gc_s,
    gc_r,
):
    zn = n // (YN * CORES)
    me = lax.axis_index("ctx")
    c = lax.rem(me, CORES)
    chip = me // CORES
    y = lax.rem(chip, YN)
    z = chip // YN
    oc = 1 - c
    oy = 1 - y
    jn = KVH // CORES
    per = HQ // KVH
    td = q_ref.shape[0]
    ct = td * CORES
    rows = per * ct
    lanes = YN * rows
    slots = cache.shape[0]
    gw = 2 * HD
    half = HQ // CORES * HD
    wide = per * HD
    ch = min(512, slots)
    units = jn * zn
    c2 = LOG2E / math.sqrt(HD)

    def zat(d):
        if zn & (zn - 1):
            return lax.rem(z + d, zn)
        out = 0
        for bit in range(zn.bit_length() - 1):
            step = 1 << bit
            out = out + lax.rem(z // step + d // step, 2) * step
        return out

    def zsrc(d):
        if zn & (zn - 1):
            return lax.rem(z - d + zn, zn)
        return zat(d)

    def dev(zz, yy, cc):
        return {"ctx": (zz * YN + yy) * CORES + cc}

    peer = dev(z, y, oc)
    ypart = dev(z, oy, c)

    def remote(src, dst, ssem, rsem, target):
        return pltpu.make_async_remote_copy(
            src_ref=src,
            dst_ref=dst,
            send_sem=ssem,
            recv_sem=rsem,
            device_id=target,
            device_id_type=pl.DeviceIdType.MESH,
        )

    def arrived(slot, sem):
        pltpu.make_async_copy(slot, slot, sem).wait()

    def cols(group):
        return pl.ds(pl.multiple_of(group * gw, gw), gw)

    local = []
    for j in range(jn):
        local.append(
            pltpu.make_async_copy(cache.at[:, cols(c * jn + j)], kvx.at[j, c], kv_sem.at[j])
        )
    for j in range(jn):
        local.append(
            pltpu.make_async_copy(nk_ref.at[:, cols(c * jn + j)], nkx.at[j, c], nk_sem.at[j])
        )
    q_half = pl.ds(pl.multiple_of(c * half, half), half)
    q_other = pl.ds(pl.multiple_of(oc * half, half), half)
    q_local = pltpu.make_async_copy(q_ref.at[:, q_half], qd.at[c], qd_sem)
    q_local.start()
    for copy in local:
        copy.start()

    barrier = pltpu.get_barrier_semaphore()
    pl.semaphore_signal(barrier, inc=1, device_id=peer, device_id_type=pl.DeviceIdType.MESH)
    pl.semaphore_signal(barrier, inc=1, device_id=ypart, device_id_type=pl.DeviceIdType.MESH)
    for d in range(1, zn):
        pl.semaphore_signal(
            barrier, inc=1, device_id=dev(zat(d), y, c), device_id_type=pl.DeviceIdType.MESH
        )
    pl.semaphore_wait(barrier, zn + 1)

    sends = []

    def send(*args):
        copy = remote(*args)
        copy.start()
        sends.append(copy)

    send(q_ref.at[:, q_other], qd.at[c], qds_sem, qdr_sem, peer)
    for j in range(jn):
        send(nk_ref.at[:, cols(oc * jn + j)], nkx.at[j, c], nks_sem.at[j], nkr_sem.at[j], peer)
        send(cache.at[:, cols(oc * jn + j)], kvx.at[j, c], kvs_sem.at[j], kvr_sem.at[j], peer)
    weights = []
    for j in range(jn):
        for k in range(CORES):
            g = k * jn + j
            copy = pltpu.make_async_copy(
                weight.at[pl.ds(g * wide, wide), :], wv.at[g], w_sem.at[g]
            )
            copy.start()
            weights.append(copy)

    q_local.wait()
    arrived(qd.at[oc], qdr_sem)
    my_rows = pl.ds(pl.multiple_of(y * rows, rows), rows)
    other_rows = pl.ds(pl.multiple_of(oy * rows, rows), rows)
    for j in range(jn):
        tiles = []
        for h in range(per):
            at = (j * per + h) * HD
            tiles.append(
                jnp.concatenate(
                    [qd[k, :, at : at + HD].astype(F32) for k in range(CORES)], axis=0
                )
            )
        qall[z, j, my_rows, :] = jnp.concatenate(tiles, axis=0).astype(BF16)

    for j in range(jn):
        mine = qall.at[z, j, my_rows]
        send(mine, mine, qy_s.at[j, 0], qy_r.at[j, 0], ypart)
        for i in range(1, zn):
            d = zn - i if j else i
            send(mine, mine, qz_s.at[j, d], qz_r.at[j, d], dev(zat(d), y, c))

    for j in range(jn):
        local[j].wait()
        local[jn + j].wait()
        arrived(nkx.at[j, oc], nkr_sem.at[j])
        fresh = [nkx[j, k].astype(F32) for k in range(CORES)]
        fresh.append(jnp.zeros((PAD - ct, gw), F32))
        nkp[j] = jnp.concatenate(fresh, axis=0).astype(BF16)
        arrived(kvx.at[j, oc], kvr_sem.at[j])
        for k in range(CORES):
            vt[j, k] = kvx[j, k, :, HD:].T

    def attend(j, d):
        zz = zsrc(d)
        q = qall[zz, j]
        lane = lax.broadcasted_iota(jnp.int32, (1, lanes), 1)
        token = lax.rem(lane, ct) + (lane // rows) * ct
        pos = jnp.zeros((1, lanes), jnp.int32)
        for t in range(YN * ct):
            pos = jnp.where(token == t, positions[zz * (YN * ct) + t], pos)
        top = jnp.full((8, lanes), LOW, F32)
        for k in range(CORES):
            live = lengths[chip * CORES + k]
            for i in range(slots // ch):
                s = lax.dot_general(
                    kvx[j, k, i * ch : (i + 1) * ch, :HD],
                    q,
                    (((1,), (1,)), ((), ())),
                    preferred_element_type=F32,
                )
                slot = lax.broadcasted_iota(jnp.int32, s.shape, 0)
                s = jnp.where(slot < live - i * ch, s, LOW)
                top = jnp.maximum(top, jnp.max(s.reshape(ch // 8, 8, lanes), axis=0))
                at = k * slots + i * ch
                sc[at : at + ch, :] = s
        row = lax.broadcasted_iota(jnp.int32, (PAD, lanes), 0)
        fresh = lax.dot_general(
            nkp[j, :, :HD], q, (((1,), (1,)), ((), ())), preferred_element_type=F32
        )
        key_pos = jnp.full((PAD, lanes), jnp.int32(2**30))
        for t in range(ct):
            key_pos = jnp.where(row == t, positions[chip * ct + t], key_pos)
        fresh = jnp.where(pos >= key_pos, fresh, LOW)
        top = jnp.maximum(top, jnp.max(fresh.reshape(PAD // 8, 8, lanes), axis=0))
        high = jnp.max(top, axis=0, keepdims=True) * c2
        total = jnp.zeros((8, lanes), F32)
        out = jnp.zeros((HD, lanes), F32)
        for k in range(CORES):
            for i in range(slots // ch):
                at = k * slots + i * ch
                p = jnp.exp2(sc[at : at + ch, :] * c2 - high)
                total = total + jnp.sum(p.reshape(ch // 8, 8, lanes), axis=0)
                out = out + jnp.dot(
                    vt[j, k, :, i * ch : (i + 1) * ch],
                    p.astype(BF16),
                    preferred_element_type=F32,
                )
        p = jnp.exp2(fresh * c2 - high)
        total = total + jnp.sum(p.reshape(PAD // 8, 8, lanes), axis=0)
        out = out + lax.dot_general(
            nkp[j, :, HD:],
            p.astype(BF16),
            (((0,), (0,)), ((), ())),
            preferred_element_type=F32,
        )
        ell = jnp.sum(total, axis=0, keepdims=True)
        packet = pack_partial(out * (1.0 / ell), high + jnp.log(ell) * LOG2E)
        u = j * zn + d
        for yy in range(YN):
            pk[u, yy] = packet[:, yy * rows : (yy + 1) * rows]
        to_partner(u).start()

    def to_partner(u):
        return remote(pk.at[u, oy], ry.at[u], ry_s.at[u], ry_r.at[u], ypart)

    def to_owner(u, d):
        return remote(zm.at[u], rz.at[u], rz_s.at[u], rz_r.at[u], dev(zsrc(d), y, c))

    def fold(j, d):
        u = j * zn + d
        arrived(ry.at[u], ry_r.at[u])
        packet = pack_partial(
            *merge_partials([unpack_partial(pk[u, y]), unpack_partial(ry[u])])
        )

        if isinstance(d, int) and d == 0:
            rz[u] = packet
            return

        @pl.when(d == 0)
        def _():
            rz[u] = packet

        @pl.when(d != 0)
        def _():
            zm[u] = packet
            to_owner(u, d).start()

    def query_relay(j, d):
        slot = qall.at[zsrc(d), j, my_rows]
        return remote(slot, slot, qy_s.at[j, d], qy_r.at[j, d], ypart)

    def relay_query(j, d):
        arrived(qall.at[zsrc(d), j, my_rows], qz_r.at[j, d])
        query_relay(j, d).start()

    def query_wait(j, d):
        arrived(qall.at[zsrc(d), j, other_rows], qy_r.at[j, d])

    def finish(j):
        for d in range(1, zn):
            arrived(rz.at[j * zn + d], rz_r.at[j * zn + d])
        out, _ = merge_partials([unpack_partial(rz[j * zn + d]) for d in range(zn)])
        out = out.T
        for h in range(per):
            ag[c, j, chip, :, h * HD : (h + 1) * HD] = out[h * ct : (h + 1) * ct].astype(BF16)
        slot = ag.at[c, j, chip]
        for d in range(1, zn):
            send(slot, slot, gz_s.at[j, d], gz_r.at[j, d], dev(zat(d), y, c))
        send(slot, slot, gy_s.at[j, 0], gy_r.at[j, 0], ypart)
        send(slot, slot, gc_s.at[j, 0, 0], gc_r.at[j, 0, 0], peer)

    def relay_along(j, start, stop):
        for d in range(start, stop):
            slot = ag.at[c, j, zsrc(d) * YN + y]
            arrived(slot, gz_r.at[j, d])
            send(slot, slot, gy_s.at[j, d], gy_r.at[j, d], ypart)
            send(slot, slot, gc_s.at[j, 0, d], gc_r.at[j, 0, d], peer)

    def relay_across(j, start, stop):
        for d in range(start, stop):
            slot = ag.at[c, j, zsrc(d) * YN + oy]
            arrived(slot, gy_r.at[j, d])
            send(slot, slot, gc_s.at[j, 1, d], gc_r.at[j, 1, d], peer)

    def project(j, k, first, last):
        width = proj_out.shape[1]
        nb = min(256, width)
        g = k * jn + j
        whole = jnp.concatenate([ag[k, j, i].astype(F32) for i in range(zn * YN)], axis=0)
        a_ref[...] = whole.astype(BF16)
        own = ag[k, j, chip].astype(F32)
        own = jnp.where(c == 0, own[:td], own[td:])
        att_out[:, pl.ds(pl.multiple_of(g * wide, wide), wide)] = own.astype(BF16)

        def column(i, carry):
            at = pl.ds(pl.multiple_of(i * nb, nb), nb)
            part = jnp.dot(a_ref[...], wv[g, :, at], preferred_element_type=F32)
            if not first:
                part = part + acc[:, at]
            if last:
                proj_out[:, at] = part.astype(BF16)
            else:
                acc[:, at] = part
            return carry

        lax.fori_loop(0, width // nb, column, 0)

    def project_peer(j):
        for d in range(zn):
            arrived(ag.at[oc, j, zsrc(d) * YN + y], gc_r.at[j, 0, d])
            arrived(ag.at[oc, j, zsrc(d) * YN + oy], gc_r.at[j, 1, d])
        project(j, oc, False, j == jn - 1)

    relay_query(0, 1)
    query_wait(0, 0)
    attend(0, 0)
    for d in range(2, zn):
        relay_query(0, d)
    query_wait(1, 0)
    attend(1, 0)

    def first_group(d, carry):
        relay_query(1, zn - d)
        query_wait(0, d)
        attend(0, d)

        @pl.when(d >= 2)
        def _():
            fold(0, d - 2)

        return carry

    def second_group(d, carry):
        query_wait(1, zn - d)
        attend(1, zn - d)

        @pl.when(d == 1)
        def _():
            fold(0, zn - 2)
            fold(0, zn - 1)

        @pl.when(d == 2)
        def _():
            fold(1, 0)

        @pl.when(d >= 3)
        def _():
            fold(1, zn - (d - 2))

        return carry

    lax.fori_loop(1, zn, first_group, 0)
    lax.fori_loop(1, zn, second_group, 0)
    for copy in weights:
        copy.wait()
    finish(0)
    fold(1, 2)
    fold(1, 1)
    relay_along(0, 1, zn)
    finish(1)
    relay_across(0, 0, zn)
    relay_along(1, 1, zn - 1)
    project(0, c, True, False)
    relay_along(1, zn - 1, zn)
    relay_across(1, 0, zn - 1)
    project_peer(0)
    relay_across(1, zn - 1, zn)
    project(1, c, False, False)
    project_peer(1)

    for copy in sends:
        copy.wait_send()

    def drain(u, carry):
        to_partner(u).wait_send()
        d = lax.rem(u, zn)

        @pl.when(d != 0)
        def _():
            to_owner(u, d).wait_send()

            query_relay(u // zn, d).wait_send()

        return carry

    lax.fori_loop(0, units, drain, 0)


def shards(queries, new_kv, prefix_cache, positions, lengths, out_weight):
    n = lax.axis_size("ctx")
    td = queries.shape[0]
    zn = n // (YN * CORES)
    jn = KVH // CORES
    per = HQ // KVH
    ct = td * CORES
    rows = per * ct
    slots = prefix_cache.shape[0]
    width = out_weight.shape[1]
    wide = per * HD
    units = jn * zn
    dma = pltpu.SemaphoreType.DMA
    scratch = [
        pltpu.VMEM((KVH, wide, width), BF16),
        pltpu.VMEM((jn, CORES, slots, 2 * HD), BF16),
        pltpu.VMEM((jn, CORES, HD, slots), BF16),
        pltpu.VMEM((jn, CORES, td, 2 * HD), BF16),
        pltpu.VMEM((jn, PAD, 2 * HD), BF16),
        pltpu.VMEM((CORES, td, HQ // CORES * HD), BF16),
        pltpu.VMEM((zn, jn, YN * rows, HD), BF16),
        pltpu.VMEM((CORES * slots, YN * rows), F32),
        pltpu.VMEM((units, YN, HD + STAT, rows), BF16),
        pltpu.VMEM((units, HD + STAT, rows), BF16),
        pltpu.VMEM((units, HD + STAT, rows), BF16),
        pltpu.VMEM((units, HD + STAT, rows), BF16),
        pltpu.VMEM((CORES, jn, zn * YN, ct, wide), BF16),
        pltpu.VMEM((td * n, wide), BF16),
        pltpu.VMEM((td * n, width), F32),
        dma((KVH,)),
        dma((jn,)),
        dma((jn,)),
        dma((jn,)),
        dma((jn,)),
        dma((jn,)),
        dma((jn,)),
        dma,
        dma,
        dma,
        dma((jn, zn)),
        dma((jn, zn)),
        dma((jn, zn)),
        dma((jn, zn)),
        dma((units,)),
        dma((units,)),
        dma((units,)),
        dma((units,)),
        dma((jn, zn)),
        dma((jn, zn)),
        dma((jn, zn)),
        dma((jn, zn)),
        dma((jn, YN, zn)),
        dma((jn, YN, zn)),
    ]
    smem = pl.BlockSpec(memory_space=pltpu.SMEM)
    vmem = pl.BlockSpec(memory_space=pltpu.VMEM)
    hbm = pl.BlockSpec(memory_space=pl.ANY)
    return pl.pallas_call(
        functools.partial(kernel, n),
        out_shape=(
            jax.ShapeDtypeStruct(queries.shape, BF16),
            jax.ShapeDtypeStruct((td * n, width), BF16),
        ),
        in_specs=[smem, smem, vmem, vmem, hbm, hbm],
        out_specs=(vmem, vmem),
        scratch_shapes=scratch,
        compiler_params=pltpu.CompilerParams(
            collective_id=0,
            has_side_effects=True,
            vmem_limit_bytes=60 * 2**20,
        ),
        name="turn_attention",
    )(positions, lengths, queries, new_kv, prefix_cache, out_weight)


def solution(mesh):
    in_specs = (
        P(("groups", "ctx"), None),
        P(("groups", "ctx"), None),
        P(("groups", "ctx"), None),
        P("groups"),
        P("groups"),
        P(None, "ctx"),
    )
    out_specs = (P(("groups", "ctx"), None), P("groups", "ctx"))
    return jax.shard_map(shards, mesh=mesh, in_specs=in_specs, out_specs=out_specs, check_vma=False)
```

```python
import functools
import math

import jax
import jax.numpy as jnp
from jax import lax
from jax.experimental import pallas as pl
from jax.experimental.pallas import tpu as pltpu
from jax.sharding import PartitionSpec as P

HQ = 64
KVH = 4
HD = 128
CORES = 2
YN = 2
PAD = 16
STAT = 16
LOW = -1e30
LOG2E = math.log2(math.e)

F32 = jnp.float32
BF16 = jnp.bfloat16


def pack_partial(o, lse):
    hi = lse.astype(BF16).astype(F32)
    mid = (lse - hi).astype(BF16).astype(F32)
    lo = lse - hi - mid
    row = lax.broadcasted_iota(jnp.int32, (STAT, o.shape[1]), 0)
    stat = jnp.where(row == 0, hi, jnp.where(row == 1, mid, lo))
    return jnp.concatenate([o.astype(BF16), stat.astype(BF16)], axis=0)


def unpack_partial(packet):
    stat = packet[HD : HD + STAT].astype(F32)
    return packet[:HD].astype(F32), stat[0:1] + stat[1:2] + stat[2:3]


def merge_partials(parts):
    top = functools.reduce(jnp.maximum, [lse for _, lse in parts])
    weights = [jnp.exp2(lse - top) for _, lse in parts]
    total = functools.reduce(jnp.add, weights)
    inverse = 1.0 / total
    out = functools.reduce(
        jnp.add, [o * (w * inverse) for (o, _), w in zip(parts, weights)]
    )
    return out, top + jnp.log(total) * LOG2E


def kernel(
    n,
    positions,
    lengths,
    q_ref,
    nk_ref,
    cache,
    weight,
    att_out,
    proj_out,
    wv,
    kvx,
    vt,
    nkx,
    nkp,
    qd,
    qall,
    sc,
    pk,
    ry,
    zm,
    rz,
    ag,
    a_ref,
    acc,
    w_sem,
    kv_sem,
    kvs_sem,
    kvr_sem,
    nk_sem,
    nks_sem,
    nkr_sem,
    qd_sem,
    qds_sem,
    qdr_sem,
    qz_s,
    qz_r,
    qy_s,
    qy_r,
    ry_s,
    ry_r,
    rz_s,
    rz_r,
    gz_s,
    gz_r,
    gy_s,
    gy_r,
    gc_s,
    gc_r,
):
    zn = n // (YN * CORES)
    me = lax.axis_index("ctx")
    c = lax.rem(me, CORES)
    chip = me // CORES
    y = lax.rem(chip, YN)
    z = chip // YN
    oc = 1 - c
    oy = 1 - y
    jn = KVH // CORES
    per = HQ // KVH
    td = q_ref.shape[0]
    ct = td * CORES
    rows = per * ct
    lanes = YN * rows
    slots = cache.shape[0]
    gw = 2 * HD
    half = HQ // CORES * HD
    wide = per * HD
    ch = min(512, slots)
    units = jn * zn
    c2 = LOG2E / math.sqrt(HD)

    def zat(d):
        if zn & (zn - 1):
            return lax.rem(z + d, zn)
        out = 0
        for bit in range(zn.bit_length() - 1):
            step = 1 << bit
            out = out + lax.rem(z // step + d // step, 2) * step
        return out

    def zsrc(d):
        if zn & (zn - 1):
            return lax.rem(z - d + zn, zn)
        return zat(d)

    def dev(zz, yy, cc):
        return {"ctx": (zz * YN + yy) * CORES + cc}

    peer = dev(z, y, oc)
    ypart = dev(z, oy, c)

    def remote(src, dst, ssem, rsem, target):
        return pltpu.make_async_remote_copy(
            src_ref=src,
            dst_ref=dst,
            send_sem=ssem,
            recv_sem=rsem,
            device_id=target,
            device_id_type=pl.DeviceIdType.MESH,
        )

    def arrived(slot, sem):
        pltpu.make_async_copy(slot, slot, sem).wait()

    def cols(group):
        return pl.ds(pl.multiple_of(group * gw, gw), gw)

    local = []
    for j in range(jn):
        local.append(
            pltpu.make_async_copy(cache.at[:, cols(c * jn + j)], kvx.at[j, c], kv_sem.at[j])
        )
    for j in range(jn):
        local.append(
            pltpu.make_async_copy(nk_ref.at[:, cols(c * jn + j)], nkx.at[j, c], nk_sem.at[j])
        )
    q_half = pl.ds(pl.multiple_of(c * half, half), half)
    q_other = pl.ds(pl.multiple_of(oc * half, half), half)
    q_local = pltpu.make_async_copy(q_ref.at[:, q_half], qd.at[c], qd_sem)
    q_local.start()
    for copy in local:
        copy.start()

    barrier = pltpu.get_barrier_semaphore()
    pl.semaphore_signal(barrier, inc=1, device_id=peer, device_id_type=pl.DeviceIdType.MESH)
    pl.semaphore_signal(barrier, inc=1, device_id=ypart, device_id_type=pl.DeviceIdType.MESH)
    for d in range(1, zn):
        pl.semaphore_signal(
            barrier, inc=1, device_id=dev(zat(d), y, c), device_id_type=pl.DeviceIdType.MESH
        )
    pl.semaphore_wait(barrier, zn + 1)

    sends = []

    def send(*args):
        copy = remote(*args)
        copy.start()
        sends.append(copy)

    send(q_ref.at[:, q_other], qd.at[c], qds_sem, qdr_sem, peer)
    for j in range(jn):
        send(nk_ref.at[:, cols(oc * jn + j)], nkx.at[j, c], nks_sem.at[j], nkr_sem.at[j], peer)
        send(cache.at[:, cols(oc * jn + j)], kvx.at[j, c], kvs_sem.at[j], kvr_sem.at[j], peer)
    weights = []
    for j in range(jn):
        for k in range(CORES):
            g = k * jn + j
            copy = pltpu.make_async_copy(
                weight.at[pl.ds(g * wide, wide), :], wv.at[g], w_sem.at[g]
            )
            copy.start()
            weights.append(copy)

    q_local.wait()
    arrived(qd.at[oc], qdr_sem)
    my_rows = pl.ds(pl.multiple_of(y * rows, rows), rows)
    other_rows = pl.ds(pl.multiple_of(oy * rows, rows), rows)
    for j in range(jn):
        tiles = []
        for h in range(per):
            at = (j * per + h) * HD
            tiles.append(
                jnp.concatenate(
                    [qd[k, :, at : at + HD].astype(F32) for k in range(CORES)], axis=0
                )
            )
        qall[z, j, my_rows, :] = jnp.concatenate(tiles, axis=0).astype(BF16)

    for j in range(jn):
        mine = qall.at[z, j, my_rows]
        send(mine, mine, qy_s.at[j, 0], qy_r.at[j, 0], ypart)
        for i in range(1, zn):
            d = zn - i if j else i
            send(mine, mine, qz_s.at[j, d], qz_r.at[j, d], dev(zat(d), y, c))

    for j in range(jn):
        local[j].wait()
        local[jn + j].wait()
        arrived(nkx.at[j, oc], nkr_sem.at[j])
        fresh = [nkx[j, k].astype(F32) for k in range(CORES)]
        fresh.append(jnp.zeros((PAD - ct, gw), F32))
        nkp[j] = jnp.concatenate(fresh, axis=0).astype(BF16)
        arrived(kvx.at[j, oc], kvr_sem.at[j])
        for k in range(CORES):
            vt[j, k] = kvx[j, k, :, HD:].T

    def attend(j, d):
        zz = zsrc(d)
        q = qall[zz, j]
        lane = lax.broadcasted_iota(jnp.int32, (1, lanes), 1)
        token = lax.rem(lane, ct) + (lane // rows) * ct
        pos = jnp.zeros((1, lanes), jnp.int32)
        for t in range(YN * ct):
            pos = jnp.where(token == t, positions[zz * (YN * ct) + t], pos)
        top = jnp.full((8, lanes), LOW, F32)
        for k in range(CORES):
            live = lengths[chip * CORES + k]
            for i in range(slots // ch):
                s = lax.dot_general(
                    kvx[j, k, i * ch : (i + 1) * ch, :HD],
                    q,
                    (((1,), (1,)), ((), ())),
                    preferred_element_type=F32,
                )
                slot = lax.broadcasted_iota(jnp.int32, s.shape, 0)
                s = jnp.where(slot < live - i * ch, s, LOW)
                top = jnp.maximum(top, jnp.max(s.reshape(ch // 8, 8, lanes), axis=0))
                at = k * slots + i * ch
                sc[at : at + ch, :] = s
        row = lax.broadcasted_iota(jnp.int32, (PAD, lanes), 0)
        fresh = lax.dot_general(
            nkp[j, :, :HD], q, (((1,), (1,)), ((), ())), preferred_element_type=F32
        )
        key_pos = jnp.full((PAD, lanes), jnp.int32(2**30))
        for t in range(ct):
            key_pos = jnp.where(row == t, positions[chip * ct + t], key_pos)
        fresh = jnp.where(pos >= key_pos, fresh, LOW)
        top = jnp.maximum(top, jnp.max(fresh.reshape(PAD // 8, 8, lanes), axis=0))
        high = jnp.max(top, axis=0, keepdims=True) * c2
        total = jnp.zeros((8, lanes), F32)
        out = jnp.zeros((HD, lanes), F32)
        for k in range(CORES):
            for i in range(slots // ch):
                at = k * slots + i * ch
                p = jnp.exp2(sc[at : at + ch, :] * c2 - high)
                total = total + jnp.sum(p.reshape(ch // 8, 8, lanes), axis=0)
                out = out + jnp.dot(
                    vt[j, k, :, i * ch : (i + 1) * ch],
                    p.astype(BF16),
                    preferred_element_type=F32,
                )
        p = jnp.exp2(fresh * c2 - high)
        total = total + jnp.sum(p.reshape(PAD // 8, 8, lanes), axis=0)
        out = out + lax.dot_general(
            nkp[j, :, HD:],
            p.astype(BF16),
            (((0,), (0,)), ((), ())),
            preferred_element_type=F32,
        )
        ell = jnp.sum(total, axis=0, keepdims=True)
        packet = pack_partial(out * (1.0 / ell), high + jnp.log(ell) * LOG2E)
        u = j * zn + d
        for yy in range(YN):
            pk[u, yy] = packet[:, yy * rows : (yy + 1) * rows]
        to_partner(u).start()

    def to_partner(u):
        return remote(pk.at[u, oy], ry.at[u], ry_s.at[u], ry_r.at[u], ypart)

    def to_owner(u, d):
        return remote(zm.at[u], rz.at[u], rz_s.at[u], rz_r.at[u], dev(zsrc(d), y, c))

    def fold(j, d):
        u = j * zn + d
        arrived(ry.at[u], ry_r.at[u])
        packet = pack_partial(
            *merge_partials([unpack_partial(pk[u, y]), unpack_partial(ry[u])])
        )

        if isinstance(d, int) and d == 0:
            rz[u] = packet
            return

        @pl.when(d == 0)
        def _():
            rz[u] = packet

        @pl.when(d != 0)
        def _():
            zm[u] = packet
            to_owner(u, d).start()

    def query_relay(j, d):
        slot = qall.at[zsrc(d), j, my_rows]
        return remote(slot, slot, qy_s.at[j, d], qy_r.at[j, d], ypart)

    def relay_query(j, d):
        arrived(qall.at[zsrc(d), j, my_rows], qz_r.at[j, d])
        query_relay(j, d).start()

    def query_wait(j, d):
        arrived(qall.at[zsrc(d), j, other_rows], qy_r.at[j, d])

    def finish(j):
        for d in range(1, zn):
            arrived(rz.at[j * zn + d], rz_r.at[j * zn + d])
        out, _ = merge_partials([unpack_partial(rz[j * zn + d]) for d in range(zn)])
        out = out.T
        for h in range(per):
            ag[c, j, chip, :, h * HD : (h + 1) * HD] = out[h * ct : (h + 1) * ct].astype(BF16)
        slot = ag.at[c, j, chip]
        for d in range(1, zn):
            send(slot, slot, gz_s.at[j, d], gz_r.at[j, d], dev(zat(d), y, c))
        send(slot, slot, gy_s.at[j, 0], gy_r.at[j, 0], ypart)
        send(slot, slot, gc_s.at[j, 0, 0], gc_r.at[j, 0, 0], peer)

    def relay_along(j, start, stop):
        for d in range(start, stop):
            slot = ag.at[c, j, zsrc(d) * YN + y]
            arrived(slot, gz_r.at[j, d])
            send(slot, slot, gy_s.at[j, d], gy_r.at[j, d], ypart)
            send(slot, slot, gc_s.at[j, 0, d], gc_r.at[j, 0, d], peer)

    def relay_across(j, start, stop):
        for d in range(start, stop):
            slot = ag.at[c, j, zsrc(d) * YN + oy]
            arrived(slot, gy_r.at[j, d])
            send(slot, slot, gc_s.at[j, 1, d], gc_r.at[j, 1, d], peer)

    def project(j, k, first, last):
        width = proj_out.shape[1]
        nb = min(256, width)
        g = k * jn + j
        whole = jnp.concatenate([ag[k, j, i].astype(F32) for i in range(zn * YN)], axis=0)
        a_ref[...] = whole.astype(BF16)
        own = ag[k, j, chip].astype(F32)
        own = jnp.where(c == 0, own[:td], own[td:])
        att_out[:, pl.ds(pl.multiple_of(g * wide, wide), wide)] = own.astype(BF16)

        def column(i, carry):
            at = pl.ds(pl.multiple_of(i * nb, nb), nb)
            part = jnp.dot(a_ref[...], wv[g, :, at], preferred_element_type=F32)
            if not first:
                part = part + acc[:, at]
            if last:
                proj_out[:, at] = part.astype(BF16)
            else:
                acc[:, at] = part
            return carry

        lax.fori_loop(0, width // nb, column, 0)

    def project_peer(j):
        for d in range(zn):
            arrived(ag.at[oc, j, zsrc(d) * YN + y], gc_r.at[j, 0, d])
            arrived(ag.at[oc, j, zsrc(d) * YN + oy], gc_r.at[j, 1, d])
        project(j, oc, False, j == jn - 1)

    relay_query(0, 1)
    query_wait(0, 0)
    attend(0, 0)
    for d in range(2, zn):
        relay_query(0, d)
    query_wait(1, 0)
    attend(1, 0)

    def first_group(d, carry):
        relay_query(1, zn - d)
        query_wait(0, d)
        attend(0, d)

        @pl.when(d >= 2)
        def _():
            fold(0, d - 2)

        return carry

    def second_group(d, carry):
        query_wait(1, zn - d)
        attend(1, zn - d)

        @pl.when(d == 1)
        def _():
            fold(0, zn - 2)
            fold(0, zn - 1)

        @pl.when(d == 2)
        def _():
            fold(1, 0)

        @pl.when(d >= 3)
        def _():
            fold(1, zn - (d - 2))

        return carry

    lax.fori_loop(1, zn, first_group, 0)
    lax.fori_loop(1, zn, second_group, 0)
    for copy in weights:
        copy.wait()
    finish(0)
    fold(1, 2)
    fold(1, 1)
    relay_along(0, 1, zn)
    finish(1)
    relay_across(0, 0, zn)
    relay_along(1, 1, zn - 1)
    project(0, c, True, False)
    relay_along(1, zn - 1, zn)
    relay_across(1, 0, zn - 1)
    project_peer(0)
    relay_across(1, zn - 1, zn)
    project(1, c, False, False)
    project_peer(1)

    for copy in sends:
        copy.wait_send()

    def drain(u, carry):
        to_partner(u).wait_send()
        d = lax.rem(u, zn)

        @pl.when(d != 0)
        def _():
            to_owner(u, d).wait_send()

            query_relay(u // zn, d).wait_send()

        return carry

    lax.fori_loop(0, units, drain, 0)


def hand_over(att, proj, att_out, proj_out):
    att_out[...] = att[...]
    proj_out[...] = proj[...]


def shards(queries, new_kv, prefix_cache, positions, lengths, out_weight):
    n = lax.axis_size("ctx")
    td = queries.shape[0]
    zn = n // (YN * CORES)
    jn = KVH // CORES
    per = HQ // KVH
    ct = td * CORES
    rows = per * ct
    slots = prefix_cache.shape[0]
    width = out_weight.shape[1]
    wide = per * HD
    units = jn * zn
    dma = pltpu.SemaphoreType.DMA
    scratch = [
        pltpu.VMEM((KVH, wide, width), BF16),
        pltpu.VMEM((jn, CORES, slots, 2 * HD), BF16),
        pltpu.VMEM((jn, CORES, HD, slots), BF16),
        pltpu.VMEM((jn, CORES, td, 2 * HD), BF16),
        pltpu.VMEM((jn, PAD, 2 * HD), BF16),
        pltpu.VMEM((CORES, td, HQ // CORES * HD), BF16),
        pltpu.VMEM((zn, jn, YN * rows, HD), BF16),
        pltpu.VMEM((CORES * slots, YN * rows), F32),
        pltpu.VMEM((units, YN, HD + STAT, rows), BF16),
        pltpu.VMEM((units, HD + STAT, rows), BF16),
        pltpu.VMEM((units, HD + STAT, rows), BF16),
        pltpu.VMEM((units, HD + STAT, rows), BF16),
        pltpu.VMEM((CORES, jn, zn * YN, ct, wide), BF16),
        pltpu.VMEM((td * n, wide), BF16),
        pltpu.VMEM((td * n, width), F32),
        dma((KVH,)),
        dma((jn,)),
        dma((jn,)),
        dma((jn,)),
        dma((jn,)),
        dma((jn,)),
        dma((jn,)),
        dma,
        dma,
        dma,
        dma((jn, zn)),
        dma((jn, zn)),
        dma((jn, zn)),
        dma((jn, zn)),
        dma((units,)),
        dma((units,)),
        dma((units,)),
        dma((units,)),
        dma((jn, zn)),
        dma((jn, zn)),
        dma((jn, zn)),
        dma((jn, zn)),
        dma((jn, YN, zn)),
        dma((jn, YN, zn)),
    ]
    smem = pl.BlockSpec(memory_space=pltpu.SMEM)
    vmem = pl.BlockSpec(memory_space=pltpu.VMEM)
    hbm = pl.BlockSpec(memory_space=pl.ANY)
    results = pl.pallas_call(
        functools.partial(kernel, n),
        out_shape=(
            jax.ShapeDtypeStruct(queries.shape, BF16),
            jax.ShapeDtypeStruct((td * n, width), BF16),
        ),
        in_specs=[smem, smem, vmem, vmem, hbm, hbm],
        out_specs=(vmem, vmem),
        scratch_shapes=scratch,
        compiler_params=pltpu.CompilerParams(
            collective_id=0,
            has_side_effects=True,
            vmem_limit_bytes=60 * 2**20,
        ),
        name="turn_attention",
    )(positions, lengths, queries, new_kv, prefix_cache, out_weight)
    return pl.pallas_call(
        hand_over,
        out_shape=tuple(jax.ShapeDtypeStruct(r.shape, r.dtype) for r in results),
        in_specs=[vmem, vmem],
        out_specs=(vmem, vmem),
        name="hand_over",
    )(*results)


def solution(mesh):
    in_specs = (
        P(("groups", "ctx"), None),
        P(("groups", "ctx"), None),
        P(("groups", "ctx"), None),
        P("groups"),
        P("groups"),
        P(None, "ctx"),
    )
    out_specs = (P(("groups", "ctx"), None), P("groups", "ctx"))
    return jax.shard_map(shards, mesh=mesh, in_specs=in_specs, out_specs=out_specs, check_vma=False)
```
